32 devices in a mesh: dp: 2 (over x), tp: 4 (over z), cp: 4 (over y, core).
Axes of the slice: x: 2, y: 2, z: 4, core: 2. Of those that a mesh axis runs over, the one named last changes fastest.
Arguments:
- hidden_in: bfloat16 [512, 4096], P(('dp', 'cp', 'tp')), parts along dimension 0
- positions: int32 [512], P(('dp', 'cp', 'tp')), parts along dimension 0
- cache_len: int32 [2], P('dp'), parts along dimension 0
- cache_k: bfloat16 [65536, 1024], P(('dp', 'cp', 'tp')), parts along dimension 0
- cache_v: bfloat16 [65536, 1024], P(('dp', 'cp', 'tp')), parts along dimension 0
- norm1_gain: bfloat16 [4096], replicated
- w_query: bfloat16 [4096, 4096], P(None, 'tp')
- w_key: bfloat16 [4096, 1024], P(None, 'tp')
- w_value: bfloat16 [4096, 1024], P(None, 'tp')
- w_out: bfloat16 [4096, 4096], P('tp')
- norm2_gain: bfloat16 [4096], replicated
- w_gate: bfloat16 [4096, 12800], P(None, 'tp')
- w_up: bfloat16 [4096, 12800], P(None, 'tp')
- w_down: bfloat16 [12800, 4096], P('tp')
Outputs:
- output: bfloat16 [512, 4096], P(('dp', 'cp', 'tp')), parts along dimension 0
There are 2 independent parts. The reference program is written for one: setup_inputs(seed, part) draws one part's arguments, and reference() takes and returns one part's arrays. A program takes and returns all parts, laid end to end along the dimension named above; an argument that names none is the same for every part.
All inputs are finite; a program needn't handle non-finite values.
Results may differ from the reference program's by a relative error of at most 0.011109.
Values are sent between devices in bfloat16 or wider.
A program may use at most 1 GiB of HBM per device.

```python
import math
import jax
import jax.numpy as jnp
from jax import lax

TOKENS = 256
PREFIX = 32768
D_MODEL = 4096
Q_HEADS = 32
KV_HEADS = 8
HEAD_DIM = 128
FFN_DIM = 12800
SHARD_COUNT = 16
SHARD_ROWS = 16
QUERY_BLOCK = 16
ROPE_BASE = 500000.0
NORM_EPS = 1e-5


def normal_draw(rand_key, out_shape, spread):
    return (jax.random.normal(rand_key, out_shape, jnp.float32) * spread).astype(jnp.bfloat16)


def setup_inputs(seed: int = 0, part: int = 0) -> dict:
    base_key = jax.random.key(seed)
    part_keys = jax.random.split(jax.random.fold_in(base_key, part), 4)
    shared_keys = jax.random.split(jax.random.key(seed + 1), 9)
    cache_len = jax.random.randint(part_keys[0], (1,), PREFIX // 16, PREFIX + 1, dtype=jnp.int32)
    row_ids = jnp.arange(TOKENS, dtype=jnp.int32)
    half_rows = SHARD_ROWS // 2
    shard_ids = row_ids // SHARD_ROWS
    within = row_ids % SHARD_ROWS
    segment = jnp.where(within < half_rows, shard_ids, 2 * SHARD_COUNT - 1 - shard_ids)
    positions = cache_len[0] + segment * half_rows + within % half_rows
    qk_std = math.log((PREFIX + TOKENS) / 4.0) ** 0.25
    width_std = D_MODEL ** -0.5
    kv_width = KV_HEADS * HEAD_DIM
    return {
        'hidden_in': normal_draw(part_keys[1], (TOKENS, D_MODEL), 1.0),
        'positions': positions,
        'cache_len': cache_len,
        'cache_k': normal_draw(part_keys[2], (PREFIX, kv_width), qk_std),
        'cache_v': normal_draw(part_keys[3], (PREFIX, kv_width), 1.0),
        'norm1_gain': (1.0 + 0.3 * jax.random.normal(shared_keys[0], (D_MODEL,), jnp.float32)).astype(jnp.bfloat16),
        'w_query': normal_draw(shared_keys[1], (D_MODEL, Q_HEADS * HEAD_DIM), qk_std * width_std),
        'w_key': normal_draw(shared_keys[2], (D_MODEL, kv_width), qk_std * width_std),
        'w_value': normal_draw(shared_keys[3], (D_MODEL, kv_width), width_std),
        'w_out': normal_draw(shared_keys[4], (Q_HEADS * HEAD_DIM, D_MODEL), 2.0 * (Q_HEADS * HEAD_DIM) ** -0.5),
        'norm2_gain': (1.0 + 0.3 * jax.random.normal(shared_keys[5], (D_MODEL,), jnp.float32)).astype(jnp.bfloat16),
        'w_gate': normal_draw(shared_keys[6], (D_MODEL, FFN_DIM), width_std),
        'w_up': normal_draw(shared_keys[7], (D_MODEL, FFN_DIM), width_std),
        'w_down': normal_draw(shared_keys[8], (FFN_DIM, D_MODEL), FFN_DIM ** -0.5),
    }


def rms_norm(hidden, norm_gain):
    values = hidden.astype(jnp.float32)
    inv_rms = lax.rsqrt(jnp.mean(values * values, axis=-1, keepdims=True) + NORM_EPS)
    return (values * inv_rms * norm_gain.astype(jnp.float32)).astype(jnp.bfloat16)


def rotary(projected, positions):
    half_dim = HEAD_DIM // 2
    inv_freq = 1.0 / (ROPE_BASE ** (jnp.arange(half_dim, dtype=jnp.float32) * (2.0 / HEAD_DIM)))
    angles = positions.astype(jnp.float32)[:, None] * inv_freq[None, :]
    expand = (angles.shape[0],) + (1,) * (projected.ndim - 2) + (half_dim,)
    cos_table = jnp.cos(angles).reshape(expand)
    sin_table = jnp.sin(angles).reshape(expand)
    first_half = projected[..., :half_dim]
    second_half = projected[..., half_dim:]
    rotated = jnp.concatenate([first_half * cos_table - second_half * sin_table, second_half * cos_table + first_half * sin_table], axis=-1)
    return rotated.astype(jnp.bfloat16)


def reference(hidden_in, positions, cache_len, cache_k, cache_v, norm1_gain, w_query, w_key, w_value, w_out, norm2_gain, w_gate, w_up, w_down):
    groups = Q_HEADS // KV_HEADS
    block_count = TOKENS // QUERY_BLOCK
    score_scale = 1.0 / math.sqrt(HEAD_DIM)
    normed = rms_norm(hidden_in, norm1_gain)
    queries = rotary(jnp.dot(normed, w_query, preferred_element_type=jnp.float32).reshape(TOKENS, KV_HEADS, groups, HEAD_DIM), positions)
    new_keys = rotary(jnp.dot(normed, w_key, preferred_element_type=jnp.float32).reshape(TOKENS, KV_HEADS, HEAD_DIM), positions)
    new_values = jnp.dot(normed, w_value, preferred_element_type=jnp.float32).astype(jnp.bfloat16).reshape(TOKENS, KV_HEADS, HEAD_DIM)
    head_keys = jnp.moveaxis(new_keys, 1, 0)
    head_values = jnp.moveaxis(new_values, 1, 0)
    cached_keys = jnp.moveaxis(cache_k.reshape(PREFIX, KV_HEADS, HEAD_DIM), 1, 0)
    cached_values = jnp.moveaxis(cache_v.reshape(PREFIX, KV_HEADS, HEAD_DIM), 1, 0)
    cache_valid = jnp.arange(PREFIX) < cache_len[0]
    query_blocks = jnp.moveaxis(queries.reshape(block_count, QUERY_BLOCK, KV_HEADS, groups, HEAD_DIM), 2, 1)
    position_blocks = positions.reshape(block_count, QUERY_BLOCK)

    def attend_block(block_item):
        block_queries, block_pos = block_item
        causal = positions[None, None, :] <= block_pos[None, :, None]

        def attend_head(head_item):
            head_queries, cache_key_head, cache_value_head, new_key_head, new_value_head = head_item
            query_wide = head_queries.astype(jnp.float32)
            cache_scores = jnp.einsum('rgd,sd->grs', query_wide, cache_key_head.astype(jnp.float32)) * score_scale
            new_scores = jnp.einsum('rgd,sd->grs', query_wide, new_key_head.astype(jnp.float32)) * score_scale
            cache_scores = jnp.where(cache_valid[None, None, :], cache_scores, -jnp.inf)
            new_scores = jnp.where(causal, new_scores, -jnp.inf)
            row_max = jnp.maximum(jnp.max(cache_scores, axis=-1, keepdims=True), jnp.max(new_scores, axis=-1, keepdims=True))
            cache_probs = jnp.exp(cache_scores - row_max)
            new_probs = jnp.exp(new_scores - row_max)
            normalizer = jnp.sum(cache_probs, axis=-1, keepdims=True) + jnp.sum(new_probs, axis=-1, keepdims=True)
            weighted = jnp.einsum('grs,sd->grd', cache_probs.astype(jnp.bfloat16).astype(jnp.float32), cache_value_head.astype(jnp.float32))
            weighted = weighted + jnp.einsum('grs,sd->grd', new_probs.astype(jnp.bfloat16).astype(jnp.float32), new_value_head.astype(jnp.float32))
            return (weighted / normalizer).astype(jnp.bfloat16)

        return lax.map(attend_head, (block_queries, cached_keys, cached_values, head_keys, head_values))

    attended = lax.map(attend_block, (query_blocks, position_blocks))
    attended = jnp.transpose(attended, (0, 3, 1, 2, 4)).reshape(TOKENS, Q_HEADS * HEAD_DIM)
    residual_mid = (hidden_in.astype(jnp.float32) + jnp.dot(attended, w_out, preferred_element_type=jnp.float32)).astype(jnp.bfloat16)
    normed_mid = rms_norm(residual_mid, norm2_gain)
    gate_proj = jnp.dot(normed_mid, w_gate, preferred_element_type=jnp.float32)
    up_proj = jnp.dot(normed_mid, w_up, preferred_element_type=jnp.float32)
    hidden_mlp = (jax.nn.silu(gate_proj) * up_proj).astype(jnp.bfloat16)
    return (residual_mid.astype(jnp.float32) + jnp.dot(hidden_mlp, w_down, preferred_element_type=jnp.float32)).astype(jnp.bfloat16)
```

```python
import functools
import math
import jax
import jax.numpy as jnp
from jax import lax
from jax.experimental import pallas as pl
from jax.experimental.pallas import tpu as pltpu
from jax.sharding import PartitionSpec as P

HEAD_DIM = 128
ROPE_BASE = 500000.0
NORM_EPS = 1e-5
MESH = pl.DeviceIdType.MESH
TP = 4
CP = 4
EXP_SCALE = math.log2(math.e) / math.sqrt(HEAD_DIM)
LOW = -3.0e38
BF = jnp.bfloat16
F32 = jnp.float32


def dev(t, c):
    return {"tp": t, "cp": c}


def entry_barrier(peers):
    barrier = pltpu.get_barrier_semaphore()
    for t, c in peers:
        pl.semaphore_signal(barrier, inc=1, device_id=dev(t, c), device_id_type=MESH)
    pl.semaphore_wait(barrier, len(peers))


def rcopy(src, dst, send, recv, t, c):
    return pltpu.make_async_remote_copy(src_ref=src, dst_ref=dst, send_sem=send, recv_sem=recv,
                                        device_id=dev(t, c), device_id_type=MESH)


def norm_rows(values, gain):
    values = values.astype(F32)
    inv_rms = lax.rsqrt(jnp.mean(values * values, axis=-1, keepdims=True) + NORM_EPS)
    return (values * inv_rms * gain.astype(F32)).astype(BF)


def qkv_kernel(rows, x_ref, g_ref, cos_ref, sin_ref, wq_hbm, wk_hbm, wv_hbm, qg_ref, k_ref, v_ref,
               wq, wk, wv, xg, act, wsem, xsend, xrecv, qsend, qrecv):
    t = lax.axis_index("tp")
    c = lax.axis_index("cp")
    group_rows = rows * TP
    wcopies = []
    for i, (src, dst) in enumerate(((wq_hbm, wq), (wk_hbm, wk), (wv_hbm, wv))):
        cp = pltpu.make_async_copy(src, dst, wsem.at[i])
        cp.start()
        wcopies.append(cp)
    zpeers = [lax.rem(t + d, TP) for d in (1, 3, 2)]
    cy = lax.rem(c + 2, CP)
    cc = c + 1 - 2 * lax.rem(c, 2)
    entry_barrier([(z, c) for z in zpeers] + [(t, cy), (t, cc)])
    sends = []
    for i, z in enumerate(zpeers):
        cp = rcopy(x_ref, xg.at[t], xsend.at[i], xrecv.at[t], z, c)
        cp.start()
        sends.append(cp)
    act[pl.ds(pl.multiple_of(t * rows, rows), rows), :] = norm_rows(x_ref[...], g_ref[...])
    for i, z in enumerate(zpeers):
        rcopy(x_ref, xg.at[z], xsend.at[i], xrecv.at[z], z, c).wait_recv()
        act[pl.ds(pl.multiple_of(z * rows, rows), rows), :] = norm_rows(xg[z], g_ref[...])
    cos = cos_ref[...]
    sin = sin_ref[...]

    def rotate(part):
        return (part * cos + pltpu.roll(part, HEAD_DIM // 2, 1) * sin).astype(BF)

    wcopies[0].wait()
    a = act[...]
    groups = wq.shape[1] // wk.shape[1]
    kv_local = wk.shape[1] // HEAD_DIM
    for kv in range(kv_local):
        width = groups * HEAD_DIM
        qh = jnp.dot(a, wq[:, kv * width:(kv + 1) * width], preferred_element_type=F32)
        for g in range(groups):
            qg_ref[c, t, kv, g * group_rows:(g + 1) * group_rows, :] = rotate(qh[:, g * HEAD_DIM:(g + 1) * HEAD_DIM])
    own = qg_ref.at[c, t]
    started = []

    def push(block, n, cb, tb, tz, cz):
        cp = rcopy(block, block, qsend.at[n], qrecv.at[cb, tb], tz, cz)
        cp.start()
        started.append(cp)

    def arrive(cb, tb):
        blk = qg_ref.at[cb, tb]
        rcopy(blk, blk, qsend.at[0], qrecv.at[cb, tb], t, cy).wait_recv()
        return blk

    n = 0
    for z in zpeers:
        push(own, n, c, t, z, c)
        n += 1
    push(own, n, c, t, t, cy)
    push(own, n + 1, c, t, t, cc)
    n += 2
    wcopies[1].wait()
    wcopies[2].wait()
    kn = jnp.dot(a, wk[...], preferred_element_type=F32)
    vn = jnp.dot(a, wv[...], preferred_element_type=F32)
    for kv in range(kv_local):
        sl = slice(kv * HEAD_DIM, (kv + 1) * HEAD_DIM)
        k_ref[:, sl] = rotate(kn[:, sl])
    v_ref[...] = vn.astype(BF)
    blk = arrive(cy, t)
    push(blk, n, cy, t, t, cc)
    n += 1
    for z in zpeers:
        blk = arrive(c, z)
        push(blk, n, c, z, t, cy)
        push(blk, n + 1, c, z, t, cc)
        n += 2
    for z in zpeers:
        blk = arrive(cy, z)
        push(blk, n, cy, z, t, cc)
        n += 1
    cd = lax.rem(cc + 2, CP)
    for z in [t] + zpeers:
        arrive(cc, z)
        arrive(cd, z)
    for cp in sends + started:
        cp.wait_send()


def merge(a_ref, b):
    a = a_ref[...]
    ma, mb = a[128:129], b[128:129]
    top = jnp.maximum(ma, mb)
    wa = jnp.exp2((ma - top) * EXP_SCALE)
    wb = jnp.exp2((mb - top) * EXP_SCALE)
    o = a[:128] * wa + b[:128] * wb
    ell = a[129:130] * wa + b[129:130] * wb
    return o, top, ell


def put(ref, o, m, ell):
    ref[0:128, :] = o
    ref[128:136, :] = jnp.concatenate([m, ell, jnp.zeros((6, m.shape[1]), F32)], axis=0)


def attn_kernel(slots, rows, len_ref, q_ref, k_hbm, v_hbm, kn_ref, vn_ref, att_ref,
                kbuf, vbuf, vt, bias, nbias, probs, dsend, drecv, ysend, yrecv, zsend, zrecv, keep,
                ksem, dss, drs, yss, yrs, zss, zrs):
    t = lax.axis_index("tp")
    c = lax.axis_index("cp")
    core = lax.rem(c, 2)
    yi = c // 2
    cy = lax.rem(c + 2, CP)
    cc = c + 1 - 2 * core
    nkv = k_hbm.shape[1] // HEAD_DIM
    per_t = nkv // TP
    group_rows = rows * TP
    nq = q_ref.shape[3]

    def head_of(step):
        return lax.rem(t + 1 + step // per_t, TP) * per_t + lax.rem(step, per_t)

    def kv_copies(step):
        h = head_of(step)
        col = pl.ds(pl.multiple_of(h * HEAD_DIM, HEAD_DIM), HEAD_DIM)
        return (pltpu.make_async_copy(k_hbm.at[:, col], kbuf.at[step], ksem.at[step, 0]),
                pltpu.make_async_copy(v_hbm.at[:, col], vbuf.at[step], ksem.at[step, 1]))

    for s in range(nkv):
        for cp in kv_copies(s):
            cp.start()
    zpeers = [lax.rem(t + d, TP) for d in (1, 2, 3)]
    entry_barrier([(z, c) for z in zpeers] + [(t, cy), (t, cc)])
    base = (c * TP + t) * slots
    slot = base + lax.broadcasted_iota(jnp.int32, (slots, HEAD_DIM), 0)
    bias[...] = jnp.where(slot < len_ref[0], 0.0, -jnp.inf).astype(F32)

    def rel(device, w):
        half = rows // 2
        seg = jnp.where(w < half, device, 2 * TP * CP - 1 - device)
        return seg * half + lax.rem(w, half)

    ki = lax.broadcasted_iota(jnp.int32, (group_rows, nq), 0)
    qi = lax.rem(lax.broadcasted_iota(jnp.int32, (group_rows, nq), 1), group_rows)
    krel = rel(c * TP + ki // rows, lax.rem(ki, rows))
    for cq in range(CP):
        qrel = rel(cq * TP + qi // rows, lax.rem(qi, rows))
        nbias[cq] = jnp.where(krel <= qrel, 0.0, -jnp.inf).astype(F32)

    def tile(step, h, cq, local):
        tq = h // per_t
        q = q_ref[cq, tq, lax.rem(h, per_t)]
        dims = (((1,), (1,)), ((), ()))
        s = lax.dot_general(kbuf[step], q, dims, preferred_element_type=F32)
        b = bias[...]
        s = s + jnp.concatenate([b] * (nq // HEAD_DIM), axis=1)
        m = jnp.maximum(jnp.max(s, axis=0, keepdims=True), LOW)
        if local is not None:
            s2 = lax.dot_general(kn_ref[:, local * HEAD_DIM:(local + 1) * HEAD_DIM], q, dims, preferred_element_type=F32)
            s2 = s2 + nbias[cq]
            m = jnp.maximum(m, jnp.max(s2, axis=0, keepdims=True))
        e = jnp.exp2((s - m) * EXP_SCALE)
        ell = jnp.sum(e, axis=0, keepdims=True)
        o = jnp.dot(vt[...], e.astype(BF), preferred_element_type=F32)
        if local is not None:
            e2 = jnp.exp2((s2 - m) * EXP_SCALE)
            ell = ell + jnp.sum(e2, axis=0, keepdims=True)
            o = o + lax.dot_general(vn_ref[:, local * HEAD_DIM:(local + 1) * HEAD_DIM], e2.astype(BF),
                                    (((0,), (0,)), ((), ())), preferred_element_type=F32)
        return o, m, ell

    def d_copy(step, j):
        return rcopy(dsend.at[step, j], drecv.at[step, j], dss.at[step, j], drs.at[step, j], t, cc)

    def y_copy(step):
        return rcopy(ysend.at[step], yrecv.at[step], yss.at[step], yrs.at[step], t, cy)

    def z_copy(step, h):
        owner = h // per_t
        return rcopy(zsend.at[step], zrecv.at[step], zss.at[step], zrs.at[step], owner, c)

    def head(step, local):
        h = head_of(step)
        for cp in kv_copies(step):
            cp.wait()
        vt[...] = vbuf[step].T
        for j in range(2):
            put(dsend.at[step, j], *tile(step, h, j * 2 + 1 - core, local))
            d_copy(step, j).start()
        put(ysend.at[step], *tile(step, h, (1 - yi) * 2 + core, local))
        put(keep.at[step], *tile(step, h, yi * 2 + core, local))
        d_copy(step, 1 - yi).wait_recv()
        put(ysend.at[step], *merge(ysend.at[step], drecv[step, 1 - yi]))
        y_copy(step).start()
        d_copy(step, yi).wait_recv()
        put(keep.at[step], *merge(keep.at[step], drecv[step, yi]))

    def finish_y(step):
        y_copy(step).wait_recv()
        put(zsend.at[step], *merge(keep.at[step], yrecv[step]))

    far = nkv - per_t

    def loop(step, carry):
        head(step, None)

        @pl.when(step > 0)
        def _():
            finish_y(step - 1)
            z_copy(step - 1, head_of(step - 1)).start()
        return carry

    lax.fori_loop(0, far, loop, 0)
    for i in range(per_t):
        head(far + i, i)
        finish_y(far + i - 1)
        if i == 0:
            z_copy(far - 1, head_of(far - 1)).start()
    finish_y(nkv - 1)
    for i in range(per_t):
        own = zsend.at[far + i]
        for d in range(TP - 1):
            step = d * per_t + i
            rcopy(zsend.at[step], zrecv.at[step], zss.at[step], zrs.at[step], zpeers[d], c).wait_recv()
            o, m, ell = merge(own, zrecv[step])
            put(own, o, m, ell)
        out = (own[0:128, :] / own[129:130, :]).T.astype(BF)
        groups = nq // group_rows
        for g in range(groups):
            hd = i * groups + g
            att_ref[:, hd * HEAD_DIM:(hd + 1) * HEAD_DIM] = out[g * group_rows:(g + 1) * group_rows, :]

    def drain(step, carry):
        for j in range(2):
            d_copy(step, j).wait_send()
        y_copy(step).wait_send()

        @pl.when(step < far)
        def _():
            z_copy(step, head_of(step)).wait_send()
        return carry

    lax.fori_loop(0, nkv, drain, 0)


def mlp_kernel(rows, gchunk, dchunk, ochunk, att_ref, x_ref, g_ref, wo_hbm, wg_hbm, wu_hbm, wd_hbm, out_ref,
               wo, wg, wu, wd, part, rs1, rs2, hid, hg, act, ubuf, wosem, gsem, dsem,
               rss, rrs, hss, hrs, r2s, r2r):
    t = lax.axis_index("tp")
    c = lax.axis_index("cp")
    width = wo_hbm.shape[1]
    ffn = wg_hbm.shape[1]
    n_o = width // ochunk
    n_g = ffn // gchunk
    n_d = width // dchunk
    gslots = wg.shape[0]
    dslots = wd.shape[0]

    def o_copy(j):
        return pltpu.make_async_copy(wo_hbm.at[:, j * ochunk:(j + 1) * ochunk], wo.at[:, j * ochunk:(j + 1) * ochunk], wosem.at[j])

    def g_copy(j):
        cols = slice(j * gchunk, (j + 1) * gchunk)
        return (pltpu.make_async_copy(wg_hbm.at[:, cols], wg.at[j % gslots], gsem.at[j, 0]),
                pltpu.make_async_copy(wu_hbm.at[:, cols], wu.at[j % gslots], gsem.at[j, 1]))

    def d_copy(j):
        return pltpu.make_async_copy(wd_hbm.at[:, j * dchunk:(j + 1) * dchunk], wd.at[j % dslots], dsem.at[j])

    for j in range(n_o):
        o_copy(j).start()
    for j in range(min(gslots, n_g)):
        for cp in g_copy(j):
            cp.start()
    for j in range(min(dslots, n_d)):
        d_copy(j).start()
    zpeers = [lax.rem(t + d, TP) for d in (2, 1, 3)]
    entry_barrier([(z, c) for z in zpeers])
    sends = []

    def row_ds(z):
        return pl.ds(pl.multiple_of(z * rows, rows), rows)

    a = att_ref[...]
    for j in range(n_o):
        cols = slice(j * ochunk, (j + 1) * ochunk)
        o_copy(j).wait()
        part[:, cols] = jnp.dot(a, wo[:, cols], preferred_element_type=F32)
        for i, z in enumerate(zpeers):
            cp = rcopy(part.at[row_ds(z), cols], rs1.at[t, :, cols], rss.at[i, j], rrs.at[t, j], z, c)
            cp.start()
            sends.append(cp)
    for j in range(n_o):
        cols = slice(j * ochunk, (j + 1) * ochunk)
        total = part[row_ds(t), cols]
        for i, z in enumerate(zpeers):
            rcopy(part.at[row_ds(z), cols], rs1.at[z, :, cols], rss.at[i, j], rrs.at[z, j], z, c).wait_recv()
            total = total + rs1[z, :, cols]
        hid[:, cols] = (x_ref[:, cols].astype(F32) + total).astype(BF)
        for i, z in enumerate(zpeers):
            cp = rcopy(hid.at[:, cols], hg.at[t, :, cols], hss.at[i, j], hrs.at[t, j], z, c)
            cp.start()
            sends.append(cp)
    act[row_ds(t), :] = norm_rows(hid[...], g_ref[...])
    for i, z in enumerate(zpeers):
        for j in range(n_o):
            cols = slice(j * ochunk, (j + 1) * ochunk)
            rcopy(hid.at[:, cols], hg.at[z, :, cols], hss.at[i, j], hrs.at[z, j], z, c).wait_recv()
        act[row_ds(z), :] = norm_rows(hg[z], g_ref[...])
    for cp in sends:
        cp.wait_send()
    b = act[...]
    for j in range(n_g):
        for cp in g_copy(j):
            cp.wait()
        gate = jnp.dot(b, wg[j % gslots], preferred_element_type=F32)
        up = jnp.dot(b, wu[j % gslots], preferred_element_type=F32)
        ubuf[:, j * gchunk:(j + 1) * gchunk] = (jax.nn.silu(gate) * up).astype(BF)
        if j + gslots < n_g:
            for cp in g_copy(j + gslots):
                cp.start()
    u = ubuf[...]
    sends = []
    for j in range(n_d):
        cols = slice(j * dchunk, (j + 1) * dchunk)
        d_copy(j).wait()
        part[:, cols] = jnp.dot(u, wd[j % dslots], preferred_element_type=F32)
        if j + dslots < n_d:
            d_copy(j + dslots).start()
        for i, z in enumerate(zpeers):
            cp = rcopy(part.at[row_ds(z), cols], rs2.at[t, :, cols], r2s.at[i, j], r2r.at[t, j], z, c)
            cp.start()
            sends.append(cp)
    for j in range(n_d):
        cols = slice(j * dchunk, (j + 1) * dchunk)
        total = part[row_ds(t), cols]
        for i, z in enumerate(zpeers):
            rcopy(part.at[row_ds(z), cols], rs2.at[z, :, cols], r2s.at[i, j], r2r.at[z, j], z, c).wait_recv()
            total = total + rs2[z, :, cols]
        out_ref[:, cols] = (hid[:, cols].astype(F32) + total).astype(BF)
    for cp in sends:
        cp.wait_send()


VM = pl.BlockSpec(memory_space=pltpu.VMEM)
SM = pl.BlockSpec(memory_space=pltpu.SMEM)
ANY = pl.BlockSpec(memory_space=pl.ANY)
DMA = pltpu.SemaphoreType.DMA


def params(cid, mib):
    return pltpu.CompilerParams(collective_id=cid, has_side_effects=True, vmem_limit_bytes=mib * 1024 * 1024)


def solution(mesh):
    token_spec = P(('dp', 'cp', 'tp'), None)
    column_spec = P(None, 'tp')
    row_spec = P('tp', None)

    def device_layer(x, pos, cache_len, cache_k, cache_v, gain1, wq, wk, wv, wo, gain2, wg, wu, wd):
        rows, width = x.shape
        group_rows = rows * TP
        kv_local = wk.shape[1] // HEAD_DIM
        groups = wq.shape[1] // wk.shape[1]
        nq = groups * group_rows
        c = lax.axis_index("cp")
        half = rows // 2
        idx = jnp.arange(group_rows, dtype=jnp.int32)
        device = c * TP + idx // rows
        within = idx % rows
        seg = jnp.where(within < half, device, 2 * TP * CP - 1 - device)
        group_pos = cache_len[0] + seg * half + within % half
        half_dim = HEAD_DIM // 2
        inv_freq = 1.0 / (ROPE_BASE ** (jnp.arange(half_dim, dtype=F32) * (2.0 / HEAD_DIM)))
        angles = group_pos.astype(F32)[:, None] * inv_freq[None, :]
        cos, sin = jnp.cos(angles), jnp.sin(angles)
        cos2 = jnp.concatenate([cos, cos], axis=1)
        sin2 = jnp.concatenate([-sin, sin], axis=1)
        qg, kn, vn = pl.pallas_call(
            functools.partial(qkv_kernel, rows),
            out_shape=(jax.ShapeDtypeStruct((CP, TP, kv_local, nq, HEAD_DIM), BF),
                       jax.ShapeDtypeStruct((group_rows, wk.shape[1]), BF),
                       jax.ShapeDtypeStruct((group_rows, wk.shape[1]), BF)),
            in_specs=[VM, VM, VM, VM, ANY, ANY, ANY],
            out_specs=(VM, VM, VM),
            scratch_shapes=[pltpu.VMEM(wq.shape, BF), pltpu.VMEM(wk.shape, BF), pltpu.VMEM(wv.shape, BF),
                            pltpu.VMEM((TP, rows, width), BF), pltpu.VMEM((group_rows, width), BF),
                            DMA((3,)), DMA((3,)), DMA((TP,)), DMA((15,)), DMA((CP, TP))],
            compiler_params=params(0, 40), name="qkv",
        )(x, gain1.reshape(1, width), cos2, sin2, wq, wk, wv)
        slots = cache_k.shape[0]
        nkv = cache_k.shape[1] // HEAD_DIM
        att = pl.pallas_call(
            functools.partial(attn_kernel, slots, rows),
            out_shape=jax.ShapeDtypeStruct((group_rows, wq.shape[1]), BF),
            in_specs=[SM, VM, ANY, ANY, VM, VM],
            out_specs=VM,
            scratch_shapes=[pltpu.VMEM((nkv, slots, HEAD_DIM), BF), pltpu.VMEM((nkv, slots, HEAD_DIM), BF),
                            pltpu.VMEM((HEAD_DIM, slots), BF), pltpu.VMEM((slots, HEAD_DIM), F32),
                            pltpu.VMEM((CP, group_rows, nq), F32), pltpu.VMEM((8, 128), BF),
                            pltpu.VMEM((nkv, 2, 136, nq), F32), pltpu.VMEM((nkv, 2, 136, nq), F32),
                            pltpu.VMEM((nkv, 136, nq), F32), pltpu.VMEM((nkv, 136, nq), F32),
                            pltpu.VMEM((nkv, 136, nq), F32), pltpu.VMEM((nkv, 136, nq), F32),
                            pltpu.VMEM((nkv, 136, nq), F32),
                            DMA((nkv, 2)), DMA((nkv, 2)), DMA((nkv, 2)), DMA((nkv,)), DMA((nkv,)),
                            DMA((nkv,)), DMA((nkv,))],
            compiler_params=params(1, 60), name="attn",
        )(cache_len, qg, cache_k, cache_v, kn, vn)
        ffn = wg.shape[1]
        gchunk, dchunk, ochunk = ffn // 5, width // 8, width // 4
        n_o, n_g, n_d = 4, 5, 8
        out = pl.pallas_call(
            functools.partial(mlp_kernel, rows, gchunk, dchunk, ochunk),
            out_shape=jax.ShapeDtypeStruct((rows, width), BF),
            in_specs=[VM, VM, VM, ANY, ANY, ANY, ANY],
            out_specs=VM,
            scratch_shapes=[pltpu.VMEM(wo.shape, BF), pltpu.VMEM((3, width, gchunk), BF), pltpu.VMEM((3, width, gchunk), BF),
                            pltpu.VMEM((3, ffn, dchunk), BF), pltpu.VMEM((group_rows, width), F32),
                            pltpu.VMEM((TP, rows, width), F32), pltpu.VMEM((TP, rows, width), F32),
                            pltpu.VMEM((rows, width), BF), pltpu.VMEM((TP, rows, width), BF),
                            pltpu.VMEM((group_rows, width), BF), pltpu.VMEM((group_rows, ffn), BF),
                            DMA((n_o,)), DMA((n_g, 2)), DMA((n_d,)),
                            DMA((3, n_o)), DMA((TP, n_o)), DMA((3, n_o)), DMA((TP, n_o)), DMA((3, n_d)), DMA((TP, n_d))],
            compiler_params=params(2, 62), name="mlp",
        )(att, x, gain2.reshape(1, width), wo, wg, wu, wd)
        return out

    return jax.shard_map(device_layer, mesh=mesh, in_specs=(token_spec, P(('dp', 'cp', 'tp')), P('dp'), token_spec, token_spec, P(), column_spec, column_spec, column_spec, row_spec, P(), column_spec, column_spec, row_spec), out_specs=token_spec, check_vma=False)
```
